32 devices in a mesh: gx: 4 (over y, x), gy: 4 (over z), gz: 2 (over core).
Axes of the slice: x: 2, y: 2, z: 4, core: 2. Of those that a mesh axis runs over, the one named last changes fastest.
Arguments:
- queries: bfloat16 [16384, 1024], P(('gx', 'gy', 'gz')), may hold values from -6 to 6
- keys: bfloat16 [16384, 1024], P(('gx', 'gy', 'gz')), may hold values from -6 to 6
- values: bfloat16 [16384, 1024], P(('gx', 'gy', 'gz')), may hold values from -6 to 6
- out_grad: bfloat16 [16384, 1024], P(('gx', 'gy', 'gz')), may hold values from -0.046875 to 0.046875
- log_decay: float32 [4, 16384], P(None, ('gx', 'gy', 'gz')), may hold values from -0.8 to 0, as said below
- saved_states: bfloat16 [32, 4, 256, 256], P(('gx', 'gy', 'gz')), may hold values from -67.5 to 67.5
Outputs:
- query_grad: bfloat16 [16384, 1024], P(('gx', 'gy', 'gz'))
- key_grad: bfloat16 [16384, 1024], P(('gx', 'gy', 'gz'))
- value_grad: bfloat16 [16384, 1024], P(('gx', 'gy', 'gz'))
The draws below stay inside these ranges and needn't reach their ends.
Inputs may be any that keep to these rules, and one draw needn't show every extreme that they name: `log_decay`: every entry is negative.
All inputs are finite; a program needn't handle non-finite values.
Results may differ from the reference program's by a relative error of at most 0.0056.
Values sent between devices are 32-bit elements; how exact they have to be, the bound alone decides.
A program may use at most 512 MiB of HBM per device.

```python
import math
import jax
import jax.numpy as jnp
from jax import lax

HEAD_GROUP = 4
HEAD_DIM = 256
WIDTH = 1024
TOK_DEV = 512
TOKEN_POSITIONS = 16384
BLOCKS = 32


def draw_log_decay(key, part):
    random_subkeys = jax.random.split(jax.random.fold_in(key, 17), 7)
    head_rank = jax.random.permutation(random_subkeys[0], HEAD_GROUP)
    fast_count = max(1, HEAD_GROUP // 2)
    fast_heads = (head_rank < fast_count)[:, None]
    slow_share = jax.random.uniform(random_subkeys[1], (HEAD_GROUP, 1), jnp.float32, 0.2, 1.0)
    slow_rate = slow_share * (0.25 * math.log(10.0)) / TOKEN_POSITIONS
    fast_rate = jax.random.uniform(random_subkeys[2], (HEAD_GROUP, 1), jnp.float32, 1.0 / 50.0, 1.0 / 30.0)
    baseline_decay_rate = jnp.where(fast_heads, fast_rate, slow_rate)
    block_multiplier = jnp.exp(jax.random.uniform(random_subkeys[3], (HEAD_GROUP, TOKEN_POSITIONS // TOK_DEV), jnp.float32, -math.log(2.0), math.log(2.0)))
    block_multiplier = jnp.repeat(block_multiplier, TOK_DEV, axis=1)
    jaggedness = jax.random.uniform(random_subkeys[4], (HEAD_GROUP, TOKEN_POSITIONS), jnp.float32, 0.5, 1.5)
    spike_positions = jax.random.randint(random_subkeys[5], (2,), 0, TOKEN_POSITIONS)
    chosen_positions = jnp.arange(TOKEN_POSITIONS, dtype=jnp.int32)
    spike_mask = jnp.any(chosen_positions[None, :] == spike_positions[:, None], axis=0)
    spike_length = jnp.log(jax.random.uniform(random_subkeys[6], (HEAD_GROUP, 1), jnp.float32, 0.5, 0.8))
    final_output = -baseline_decay_rate * block_multiplier * jaggedness + jnp.where(spike_mask[None, :], spike_length, 0.0)
    return final_output.astype(jnp.float32)


def block_scale(own_key, shape, cuts, smallest, high):
    level = 1.0
    for axis_at, shards_of in cuts:
        steps = jax.random.uniform(jax.random.fold_in(jax.random.fold_in(own_key, 6), axis_at), (shards_of,), jnp.float32, smallest / len(cuts), high / len(cuts))
        level = level * jnp.repeat(jnp.exp(steps), shape[axis_at] // shards_of).reshape((-1,) + (1,) * (len(shape) - 1 - axis_at))
    return level


def normal_values(own_key, extent, scale, limit, shards=(), held_as=jnp.bfloat16):
    values = scale * jax.random.normal(own_key, extent, jnp.float32)
    if shards:
        values = values * block_scale(own_key, extent, shards, -0.22, 0.18)
    return jnp.clip(values, -limit, limit).astype(held_as)


def setup_inputs(seed: int = 0) -> dict:
    splits = jax.random.split(jax.random.key(seed), 7)
    return {
        "queries": normal_values(splits[0], (TOKEN_POSITIONS, WIDTH), 1.0, 6.0, ((0, 32),)),
        "keys": normal_values(splits[1], (TOKEN_POSITIONS, WIDTH), 1.0, 6.0, ((0, 32),)),
        "values": normal_values(splits[2], (TOKEN_POSITIONS, WIDTH), 1.0, 6.0, ((0, 32),)),
        "out_grad": normal_values(splits[3], (TOKEN_POSITIONS, WIDTH), (TOKEN_POSITIONS ** -0.5), 0.046875, ((0, 32),)),
        "log_decay": draw_log_decay(jax.random.fold_in(splits[6], 71), 0),
        "saved_states": normal_values(splits[5], (BLOCKS, HEAD_GROUP, HEAD_DIM, HEAD_DIM), (0.5 * TOK_DEV ** 0.5), 67.5, ((0, 32),)),
    }


def reference(queries, keys, values, out_grad, log_decay, saved_states):
    count_blocks = TOKEN_POSITIONS // TOK_DEV
    score_scale = HEAD_DIM ** -0.5

    def blocked(array):
        return array.reshape(count_blocks, TOK_DEV, HEAD_GROUP, HEAD_DIM)

    decay_blocks = log_decay.reshape(HEAD_GROUP, count_blocks, TOK_DEV).transpose(1, 0, 2)
    inputs = (blocked(queries), blocked(keys), blocked(values), blocked(out_grad), decay_blocks, saved_states)
    zero_state = jnp.zeros((HEAD_GROUP, HEAD_DIM, HEAD_DIM), jnp.float32)
    positions = jnp.arange(TOK_DEV, dtype=jnp.int32)
    causal = positions[:, None] >= positions[None, :]

    def backward_step(carry, block_in):
        query_heads, key_heads, value_heads, grad_heads, decay_rows, state_in = block_in
        query_f = query_heads.astype(jnp.float32)
        key_f = key_heads.astype(jnp.float32)
        value_f = value_heads.astype(jnp.float32)
        grad_f = grad_heads.astype(jnp.float32)
        cumulative = jnp.cumsum(decay_rows, axis=1)
        block_end = cumulative[:, -1:]
        to_end = jnp.exp(block_end - cumulative)
        from_start = jnp.exp(cumulative)
        log_gaps = cumulative[:, :, None] - cumulative[:, None, :]
        weight = jnp.where(causal[None], jnp.exp(jnp.minimum(log_gaps, 0.0)), 0.0)
        probs = (jnp.einsum('thd,shd->hts', query_f, key_f) * score_scale * weight).astype(jnp.bfloat16)
        grad_scores = (jnp.einsum('thd,shd->hts', grad_f, value_f) * score_scale * weight).astype(jnp.bfloat16)
        query_decayed = (query_f * (score_scale * from_start).T[:, :, None]).astype(jnp.bfloat16)
        local_grad = jnp.einsum('thi,thj->hij', query_decayed.astype(jnp.float32), grad_f)
        grad_in = carry.astype(jnp.bfloat16).astype(jnp.float32)
        state_f = state_in.astype(jnp.float32)
        probs_f = probs.astype(jnp.float32)
        grad_scores_f = grad_scores.astype(jnp.float32)
        query_grad = jnp.einsum('hts,shd->thd', grad_scores_f, key_f)
        query_grad = query_grad + jnp.einsum('thj,hij->thi', grad_f, state_f) * (score_scale * from_start).T[:, :, None]
        key_grad = jnp.einsum('hts,thd->shd', grad_scores_f, query_f)
        key_grad = key_grad + jnp.einsum('thj,hij->thi', value_f, grad_in) * to_end.T[:, :, None]
        value_grad = jnp.einsum('hts,thd->shd', probs_f, grad_f)
        value_grad = value_grad + jnp.einsum('thi,hij->thj', key_f, grad_in) * to_end.T[:, :, None]
        new_carry = jnp.exp(block_end[:, 0])[:, None, None] * carry + local_grad
        return new_carry, (query_grad.astype(jnp.bfloat16), key_grad.astype(jnp.bfloat16), value_grad.astype(jnp.bfloat16))

    last_carry, grads = lax.scan(backward_step, zero_state, inputs, reverse=True)
    query_grad = grads[0].reshape(TOKEN_POSITIONS, WIDTH)
    key_grad = grads[1].reshape(TOKEN_POSITIONS, WIDTH)
    value_grad = grads[2].reshape(TOKEN_POSITIONS, WIDTH)
    return (query_grad, key_grad, value_grad)
```

```python
import functools

import jax
import jax.numpy as jnp
from jax import lax
from jax.experimental import pallas as pl
from jax.experimental.pallas import tpu as pltpu
from jax.sharding import PartitionSpec as P

MESH = pl.DeviceIdType.MESH
F32 = jnp.float32
BF16 = jnp.bfloat16
CHUNKS = 8
DELAY = 2
TILE = 256
NT = (((1,), (1,)), ((), ()))
TN = (((0,), (0,)), ((), ()))
NN = (((1,), (0,)), ((), ()))
LX, FA, FB, RU, RD, FF, FX = 0, 2, 4, 6, 8, 10, 12


def dot(a, b, dims):
    return lax.dot_general(a, b, dims, preferred_element_type=F32)


def kernel(
    sizes, line, steps,
    q_hbm, k_hbm, v_hbm, g_hbm, ld_ref, st_hbm,
    dq_hbm, dk_hbm, dv_hbm,
    q, k, v, g, st, dq, dk, dv, dkacc, dvacc,
    brow, bcol, bend, dvm, gin,
    rbuf, rdec, lsend, ldec, lone, lown, sbuf, done_dec, dchip, tbuf, tdec, xs, xdec, oafter, obuf, gsend, fs,
    in_sem, out_sem, send_sem, recv_sem, dsend_sem, drecv_sem,
):
    gx, gy, gz = sizes
    rows_n, width = q.shape
    heads = ld_ref.shape[0]
    hd = width // heads
    scale = hd ** (-0.5)
    mid = line // 2
    rc = hd // CHUNKS

    lin = (lax.axis_index("gx") * gy + lax.axis_index("gy")) * gz + lax.axis_index("gz")
    core = lin % 2
    chip = lin // 2
    p = chip % line
    col = chip // line

    def dev(core_, p_, col_):
        at = (col_ * line + p_) * 2 + core_
        return (at // (gy * gz), (at // gz) % gy, at % gz)

    def column_partner(s):
        bit = (col // (2**s)) % 2
        return col + (1 - 2 * bit) * (2**s)

    partner = dev(1 - core, p, col)
    up = dev(core, jnp.minimum(p + 1, line - 1), col)
    down = dev(core, jnp.maximum(p - 1, 0), col)
    across = [dev(core, p, column_partner(s)) for s in range(steps)]

    loads = [
        pltpu.make_async_copy(a, b, in_sem.at[n])
        for n, (a, b) in enumerate(
            [(q_hbm, q), (g_hbm, g), (k_hbm, k), (v_hbm, v), (st_hbm.at[0], st)]
        )
    ]
    for load in loads:
        load.start()

    barrier = pltpu.get_barrier_semaphore()

    def greet(to):
        pl.semaphore_signal(barrier, inc=1, device_id=to, device_id_type=MESH)

    greet(partner)
    for s in range(steps):
        greet(across[s])

    @pl.when(p > 0)
    def _():
        greet(down)

    @pl.when(p < line - 1)
    def _():
        greet(up)

    x = ld_ref[...]
    x = jnp.concatenate([x] * (8 // heads), axis=0)
    lane = lax.broadcasted_iota(jnp.int32, x.shape, 1)
    shift = 1
    while shift < rows_n:
        x = x + jnp.where(lane >= shift, pltpu.roll(x, shift, 1), 0.0)
        shift *= 2
    columns = x.T
    end = x[:, rows_n - 1 :]
    for h in range(heads):
        bcol[h] = jnp.broadcast_to(columns[:, h : h + 1], (rows_n, 128))
        bend[h] = jnp.broadcast_to(end[h : h + 1, :], (8, 128))
        brow[h] = jnp.broadcast_to(x[h : h + 1, :], (8, rows_n))
        dvm[h] = jnp.broadcast_to(jnp.exp(end[h : h + 1, :]), (8, hd))

    def wide(a):
        return jnp.concatenate([a] * (hd // 128), axis=1)

    def cols(h):
        return pl.ds(pl.multiple_of(h * hd, hd), hd)

    def local(h):
        start = wide(scale * jnp.exp(bcol[h]))
        decayed = (q[:, cols(h)].astype(F32) * start).astype(BF16)
        return dot(decayed, g[:, cols(h)], TN)

    def decay_of(h):
        return dvm[h]

    def rows(c):
        return pl.ds(pl.multiple_of(c * rc, rc), rc)

    def chunk_copy(src, flow, c, to):
        return pltpu.make_async_remote_copy(
            src_ref=src.at[rows(c)], dst_ref=rbuf.at[flow, rows(c)],
            send_sem=send_sem.at[flow, c], recv_sem=recv_sem.at[flow, c],
            device_id=to, device_id_type=MESH,
        )

    def decay_copy(src, flow, to):
        return pltpu.make_async_remote_copy(
            src_ref=src, dst_ref=rdec.at[flow],
            send_sem=dsend_sem.at[flow], recv_sem=drecv_sem.at[flow],
            device_id=to, device_id_type=MESH,
        )

    def head_copy(src, flow, to):
        return pltpu.make_async_remote_copy(
            src_ref=src, dst_ref=rbuf.at[flow],
            send_sem=send_sem.at[flow, 0], recv_sem=recv_sem.at[flow, 0],
            device_id=to, device_id_type=MESH,
        )

    def send(src, flow, c, to, dec=None):
        if dec is not None:

            @pl.when(c == 0)
            def _():
                decay_copy(dec, flow, to).start()

        chunk_copy(src, flow, c, to).start()

    def recv(flow, c, dec=False):
        if dec:

            @pl.when(c == 0)
            def _():
                decay_copy(rdec.at[flow], flow, partner).wait_recv()

        chunk_copy(rbuf.at[flow], flow, c, partner).wait_recv()

    loads[0].wait()
    loads[1].wait()
    for j in range(2):
        other = 2 * (1 - core) + j
        lsend[j] = local(other)
        ldec[j] = decay_of(other)
        if j == 0:
            ends = (p > 0).astype(jnp.int32) + (p < line - 1).astype(jnp.int32)
            pl.semaphore_wait(barrier, 1 + steps + ends)

        decay_copy(ldec.at[j], LX + j, partner).start()
        head_copy(lsend.at[j], LX + j, partner).start()
    for j in range(2):
        lown[j] = local(2 * core + j)
    for j in range(2):
        mine = decay_of(2 * core + j)
        decay_copy(ldec.at[j], LX + j, partner).wait_recv()
        head_copy(lsend.at[j], LX + j, partner).wait_recv()
        theirs = rdec[LX + j]
        dchip[j] = mine * theirs

        @pl.when(core == 0)
        def _():
            lone[j] = rbuf[LX + j]
            sbuf[j] = lown[j] + mine[:1] * rbuf[LX + j]
            done_dec[j] = theirs

        @pl.when(core == 1)
        def _():
            lone[j] = lown[j]
            sbuf[j] = rbuf[LX + j] + theirs[:1] * lown[j]
            done_dec[j] = mine

    for load in loads[2:]:
        load.wait()

    tiles = rows_n // TILE

    def block(h, r):
        hs = cols(h)
        at = slice(r * TILE, (r + 1) * TILE)
        extent = (r + 1) * TILE
        qt, gt = q[at, hs], g[at, hs]
        ks, vs = k[:extent, hs], v[:extent, hs]
        bt = bcol[h, at, :]
        weights = []
        for n in range(extent // 128):
            gap = bt - brow[h, :1, pl.ds(n * 128, 128)]
            weight = jnp.exp(jnp.minimum(gap, 0.0))
            if (n + 1) * 128 > r * TILE:
                ti = lax.broadcasted_iota(jnp.int32, gap.shape, 0) + r * TILE
                si = lax.broadcasted_iota(jnp.int32, gap.shape, 1) + n * 128
                weight = jnp.where(ti >= si, weight, 0.0)
            weights.append(weight)
        weight = jnp.concatenate(weights, axis=1)
        probs = (dot(qt, ks, NT) * scale * weight).astype(BF16)
        gscores = (dot(gt, vs, NT) * scale * weight).astype(BF16)
        start = wide(scale * jnp.exp(bt))
        dqt = dot(gscores, ks, NN) + dot(gt, st[h], NT) * start
        dq[at, hs] = dqt.astype(BF16)
        dkp = dot(gscores, qt, TN)
        dvp = dot(probs, gt, TN)
        if r:
            dkacc[: r * TILE, hs] += dkp[: r * TILE]
            dvacc[: r * TILE, hs] += dvp[: r * TILE]
        dkacc[at, hs] = dkp[r * TILE :]
        dvacc[at, hs] = dvp[r * TILE :]

    def finish(j, c, grad):
        at = rows(c)
        alt = lone[j, at] + done_dec[j, :1] * grad
        first = core == 0
        gin[2 * core + j, at] = jnp.where(first, alt, grad).astype(BF16)
        fs[j, at] = jnp.where(first, grad, alt)
        send(fs.at[j], FF + j, c, partner)

    def step(t, carry):
        for j in range(2):
            own = mid - 1 + j

            c = t - DELAY * (mid + steps + jnp.abs(p - own))
            ok = (c >= 0) & (c < CHUNKS)

            @pl.when(ok & (p > own))
            def _():
                recv(RU + j, c)
                at = rows(c)

                @pl.when(p < line - 1)
                def _():
                    send(rbuf.at[RU + j], RU + j, c, up)
                    finish(j, c, rbuf[FA + j, at] + rdec[FA + j, :1] * rbuf[RU + j, at])

                @pl.when(p == line - 1)
                def _():
                    finish(j, c, rbuf[RU + j, at])

            @pl.when(ok & (p < own))
            def _():
                recv(RD + j, c)
                at = rows(c)

                @pl.when(p > 0)
                def _():
                    gsend[j, at] = sbuf[j, at] + dchip[j, :1] * rbuf[RD + j, at]
                    send(gsend.at[j], RD + j, c, down)

                finish(j, c, rbuf[RD + j, at])

            for s in reversed(range(steps)):
                c = t - DELAY * (mid + 1 + s)

                @pl.when((c >= 0) & (c < CHUNKS) & (p == own))
                def _():
                    recv(FX + s, c, True)
                    at = rows(c)
                    later = (col // (2**s)) % 2 == 0

                    @pl.when(c == 0)
                    def _():
                        oafter[s + 1] = jnp.where(later, oafter[s] * rdec[FX + s], oafter[s])
                        if s < steps - 1:
                            xdec[s + 1] = xdec[s] * rdec[FX + s]

                    theirs, mine = rbuf[FX + s, at], xs[s, at]
                    total = obuf[at] + jnp.where(later, oafter[s, :1] * theirs, 0.0)
                    obuf[at] = total
                    if s < steps - 1:
                        xs[s + 1, at] = jnp.where(
                            later, mine + xdec[s, :1] * theirs, theirs + rdec[FX + s, :1] * mine
                        )
                        send(xs.at[s + 1], FX + s + 1, c, across[s + 1], xdec.at[s + 1])
                    else:
                        send(obuf, RU + j, c, up)
                        grad = rbuf[FA + j, at] + rdec[FA + j, :1] * total
                        gsend[j, at] = sbuf[j, at] + dchip[j, :1] * grad
                        send(gsend.at[j], RD + j, c, down)
                        finish(j, c, grad)

            stage = jnp.where(p > own, line - 1 - p, jnp.where(p < own, p, mid))
            c = t - DELAY * stage
            ok = (c >= 0) & (c < CHUNKS)

            @pl.when(ok & (p > own))
            def _():
                at = rows(c)

                @pl.when(p < line - 1)
                def _():
                    recv(FA + j, c, True)

                    @pl.when(c == 0)
                    def _():
                        tdec[j] = dchip[j] * rdec[FA + j]

                    tbuf[j, at] = sbuf[j, at] + dchip[j, :1] * rbuf[FA + j, at]

                @pl.when(p == line - 1)
                def _():
                    @pl.when(c == 0)
                    def _():
                        tdec[j] = dchip[j]

                    tbuf[j, at] = sbuf[j, at]

                send(tbuf.at[j], FA + j, c, down, tdec.at[j])

            @pl.when(ok & (p < own))
            def _():
                at = rows(c)

                @pl.when(p > 0)
                def _():
                    recv(FB + j, c, True)

                    @pl.when(c == 0)
                    def _():
                        tdec[j] = dchip[j] * rdec[FB + j]

                    tbuf[j, at] = rbuf[FB + j, at] + rdec[FB + j, :1] * sbuf[j, at]

                @pl.when(p == 0)
                def _():
                    @pl.when(c == 0)
                    def _():
                        tdec[j] = dchip[j]

                    tbuf[j, at] = sbuf[j, at]

                send(tbuf.at[j], FB + j, c, up, tdec.at[j])

            @pl.when(ok & (p == own))
            def _():
                at = rows(c)
                recv(FA + j, c, True)
                recv(FB + j, c, True)

                @pl.when(c == 0)
                def _():
                    xdec[0] = rdec[FB + j] * dchip[j] * rdec[FA + j]
                    oafter[0] = jnp.ones_like(oafter[0])

                whole = sbuf[j, at] + dchip[j, :1] * rbuf[FA + j, at]
                xs[0, at] = rbuf[FB + j, at] + rdec[FB + j, :1] * whole
                obuf[at] = jnp.zeros((rc, hd), F32)
                send(xs.at[0], FX, c, across[0], xdec.at[0])

        for r in range(tiles):

            @pl.when((t < heads * tiles) & (t % tiles == r))
            def _():
                block(t // tiles, r)

        return carry

    last = CHUNKS + DELAY * (mid + steps + mid)
    lax.fori_loop(0, max(last, heads * tiles), step, 0)

    outs = [pltpu.make_async_copy(dq, dq_hbm, out_sem.at[0])]
    outs[0].start()

    def final(n, h):
        hs = cols(h)
        to_end = wide(jnp.exp(bend[h, :1] - bcol[h]))
        dk[:, hs] = (dkacc[:, hs] + dot(v[:, hs], gin[h], NT) * to_end).astype(BF16)
        outs.append(pltpu.make_async_copy(dk.at[:, hs], dk_hbm.at[:, hs], out_sem.at[1 + 2 * n]))
        outs[-1].start()
        dv[:, hs] = (dvacc[:, hs] + dot(k[:, hs], gin[h], NN) * to_end).astype(BF16)
        outs.append(pltpu.make_async_copy(dv.at[:, hs], dv_hbm.at[:, hs], out_sem.at[2 + 2 * n]))
        outs[-1].start()

    for j in range(2):
        final(j, 2 * core + j)
    for j in range(2):
        for c in range(CHUNKS):
            recv(FF + j, c)
        gin[2 * (1 - core) + j] = rbuf[FF + j].astype(BF16)
        final(2 + j, 2 * (1 - core) + j)

    def sent(flow, src, dec=None):
        if dec is not None:
            decay_copy(dec, flow, partner).wait_send()
        for c in range(CHUNKS):
            chunk_copy(src, flow, c, partner).wait_send()

    for j in range(2):
        own = mid - 1 + j
        decay_copy(ldec.at[j], LX + j, partner).wait_send()
        head_copy(lsend.at[j], LX + j, partner).wait_send()
        sent(FF + j, fs.at[j])

        @pl.when(p > own)
        def _():
            sent(FA + j, tbuf.at[j], tdec.at[j])

        @pl.when(p < own)
        def _():
            sent(FB + j, tbuf.at[j], tdec.at[j])

        @pl.when((p >= own) & (p < line - 1))
        def _():
            sent(RU + j, obuf)

        @pl.when((p <= own) & (p > 0))
        def _():
            sent(RD + j, gsend.at[j])

        @pl.when(p == own)
        def _():
            for s in range(steps):
                sent(FX + s, xs.at[s], xdec.at[s])

    for out in outs:
        out.wait()


def solution(mesh):
    sizes = tuple(mesh.shape[a] for a in ("gx", "gy", "gz"))
    gx, gy, gz = sizes
    line = gz // 2 if gz > 2 else gy
    columns = gx * gy * gz // (2 * line)
    steps = columns.bit_length() - 1
    assert line % 2 == 0 and line >= 4 and columns == 2**steps and steps >= 1

    def body(queries, keys, values, out_grad, log_decay, saved_states):
        n, width = queries.shape
        heads = log_decay.shape[0]
        hd = width // heads
        assert heads == 4
        flows = FX + steps
        any_ = pl.BlockSpec(memory_space=pl.ANY)
        hbm = pl.BlockSpec(memory_space=pltpu.HBM)
        state = (hd, hd)
        tile = (8, hd)
        out = jax.ShapeDtypeStruct((n, width), BF16)
        vm = pltpu.VMEM
        return pl.pallas_call(
            functools.partial(kernel, sizes, line, steps),
            out_shape=(out, out, out),
            in_specs=[hbm] * 4 + [pl.BlockSpec(memory_space=pltpu.VMEM), hbm],
            out_specs=(any_,) * 3,
            scratch_shapes=[
                vm((n, width), BF16), vm((n, width), BF16), vm((n, width), BF16), vm((n, width), BF16),
                vm((heads,) + state, BF16),
                vm((n, width), BF16), vm((n, width), BF16), vm((n, width), BF16),
                vm((n, width), F32), vm((n, width), F32),
                vm((heads, 8, n), F32), vm((heads, n, 128), F32), vm((heads, 8, 128), F32), vm((heads,) + tile, F32),
                vm((heads,) + state, BF16),
                vm((flows,) + state, F32), vm((flows,) + tile, F32),
                vm((2,) + state, F32), vm((2,) + tile, F32),
                vm((2,) + state, F32), vm((2,) + state, F32), vm((2,) + state, F32),
                vm((2,) + tile, F32), vm((2,) + tile, F32),
                vm((2,) + state, F32), vm((2,) + tile, F32),
                vm((steps,) + state, F32), vm((steps,) + tile, F32), vm((steps + 1,) + tile, F32),
                vm(state, F32), vm((2,) + state, F32), vm((2,) + state, F32),
                pltpu.SemaphoreType.DMA((5,)), pltpu.SemaphoreType.DMA((1 + 2 * heads,)),
                pltpu.SemaphoreType.DMA((flows, CHUNKS)), pltpu.SemaphoreType.DMA((flows, CHUNKS)),
                pltpu.SemaphoreType.DMA((flows,)), pltpu.SemaphoreType.DMA((flows,)),
            ],
            compiler_params=pltpu.CompilerParams(
                collective_id=0, has_side_effects=True, vmem_limit_bytes=60 * 1024 * 1024
            ),
        )(queries, keys, values, out_grad, log_decay, saved_states)

    seq = ("gx", "gy", "gz")
    return jax.shard_map(
        body,
        mesh=mesh,
        in_specs=(P(seq, None),) * 4 + (P(None, seq), P(seq, None, None, None)),
        out_specs=(P(seq, None),) * 3,
        check_vma=False,
    )
```

```python
import functools

import jax
import jax.numpy as jnp
from jax import lax
from jax.experimental import pallas as pl
from jax.experimental.pallas import tpu as pltpu
from jax.sharding import PartitionSpec as P

MESH = pl.DeviceIdType.MESH
F32 = jnp.float32
BF16 = jnp.bfloat16
PIECES = 4
PER_PIECE = 4
DELAY = 3
TILE = 256
NT = (((1,), (1,)), ((), ()))
TN = (((0,), (0,)), ((), ()))
NN = (((1,), (0,)), ((), ()))
LX, FA, FB, RU, RD, FF, FX = 0, 2, 4, 6, 8, 10, 12
DL, DA, DB, DX = 0, 2, 2 + PIECES, 2 + 2 * PIECES
CHUNKS = PIECES * PER_PIECE // 2


def dot(a, b, dims):
    return lax.dot_general(a, b, dims, preferred_element_type=F32)


def kernel(
    sizes, line, steps,
    q_hbm, k_hbm, v_hbm, g_hbm, ld_ref, st_hbm,
    dq, dk, dv,
    q, k, v, g, st, dkacc, dvacc,
    brow, bcol, bend, dvm, gin,
    rbuf, rdec, lsend, ldec, lone, lown, sbuf, done_dec, dchip, tbuf, tdec, xs, xdec, oafter, obuf, gsend, fs,
    in_sem, send_sem, recv_sem, dsend_sem, drecv_sem,
):
    gx, gy, gz = sizes
    rows_n, width = q.shape
    heads = ld_ref.shape[0]
    hd = width // heads
    scale = hd ** (-0.5)
    rc = hd // CHUNKS

    lin = (lax.axis_index("gx") * gy + lax.axis_index("gy")) * gz + lax.axis_index("gz")
    core = lin % 2
    chip = lin // 2
    p = chip % line
    col = chip // line

    def dev(core_, p_, col_):
        at = (col_ * line + p_) * 2 + core_
        return (at // (gy * gz), (at // gz) % gy, at % gz)

    def column_partner(s):
        bit = (col // (2**s)) % 2
        return col + (1 - 2 * bit) * (2**s)

    partner = dev(1 - core, p, col)
    up = dev(core, jnp.minimum(p + 1, line - 1), col)
    down = dev(core, jnp.maximum(p - 1, 0), col)
    across = [dev(core, p, column_partner(s)) for s in range(steps)]

    loads = [
        pltpu.make_async_copy(a, b, in_sem.at[n])
        for n, (a, b) in enumerate(
            [(q_hbm, q), (g_hbm, g), (k_hbm, k), (v_hbm, v), (st_hbm.at[0], st)]
        )
    ]
    for load in loads:
        load.start()

    barrier = pltpu.get_barrier_semaphore()

    def greet(to):
        pl.semaphore_signal(barrier, inc=1, device_id=to, device_id_type=MESH)

    greet(partner)
    for s in range(steps):
        greet(across[s])

    @pl.when(p > 0)
    def _():
        greet(down)

    @pl.when(p < line - 1)
    def _():
        greet(up)

    x = ld_ref[...]
    x = jnp.concatenate([x] * (8 // heads), axis=0)
    lane = lax.broadcasted_iota(jnp.int32, x.shape, 1)
    shift = 1
    while shift < rows_n:
        x = x + jnp.where(lane >= shift, pltpu.roll(x, shift, 1), 0.0)
        shift *= 2
    columns = x.T
    end = x[:, rows_n - 1 :]
    for h in range(heads):
        bcol[h] = jnp.broadcast_to(columns[:, h : h + 1], (rows_n, 128))
        bend[h] = jnp.broadcast_to(end[h : h + 1, :], (8, 128))
        brow[h] = jnp.broadcast_to(x[h : h + 1, :], (8, rows_n))
        dvm[h] = jnp.broadcast_to(jnp.exp(end[h : h + 1, :]), (8, hd))

    def wide(a):
        return jnp.concatenate([a] * (hd // 128), axis=1)

    def cols(h):
        return pl.ds(pl.multiple_of(h * hd, hd), hd)

    def local(h):
        start = wide(scale * jnp.exp(bcol[h]))
        decayed = (q[:, cols(h)].astype(F32) * start).astype(BF16)
        return dot(decayed, g[:, cols(h)], TN)

    def decay_of(h):
        return dvm[h]

    def rows(c):
        return pl.ds(pl.multiple_of(c * rc, rc), rc)

    def chunk_copy(src, flow, c, to):
        return pltpu.make_async_remote_copy(
            src_ref=src.at[rows(c)], dst_ref=rbuf.at[flow, rows(c)],
            send_sem=send_sem.at[flow, c], recv_sem=recv_sem.at[flow, c],
            device_id=to, device_id_type=MESH,
        )

    def decay_copy(src, flow, to):
        return pltpu.make_async_remote_copy(
            src_ref=src, dst_ref=rdec.at[flow],
            send_sem=dsend_sem.at[flow], recv_sem=drecv_sem.at[flow],
            device_id=to, device_id_type=MESH,
        )

    def head_copy(src, flow, to):
        return pltpu.make_async_remote_copy(
            src_ref=src, dst_ref=rbuf.at[flow],
            send_sem=send_sem.at[flow, 0], recv_sem=recv_sem.at[flow, 0],
            device_id=to, device_id_type=MESH,
        )

    def send(src, flow, c, to):
        chunk_copy(src, flow, c, to).start()

    def recv(flow, c):
        chunk_copy(rbuf.at[flow], flow, c, partner).wait_recv()

    def recv_decay(flow):
        decay_copy(rdec.at[flow], flow, partner).wait_recv()

    loads[0].wait()
    loads[1].wait()
    for j in range(2):
        other = 2 * (1 - core) + j
        lsend[j] = local(other)
        ldec[j] = decay_of(other)
        if j == 0:
            ends = (p > 0).astype(jnp.int32) + (p < line - 1).astype(jnp.int32)
            pl.semaphore_wait(barrier, 1 + steps + ends)

        decay_copy(ldec.at[j], DL + j, partner).start()
        head_copy(lsend.at[j], LX + j, partner).start()
    for j in range(2):
        lown[j] = local(2 * core + j)
    for j in range(2):
        mine = decay_of(2 * core + j)
        decay_copy(ldec.at[j], DL + j, partner).wait_recv()
        head_copy(lsend.at[j], LX + j, partner).wait_recv()
        theirs = rdec[DL + j]
        dchip[j] = mine * theirs

        @pl.when(core == 0)
        def _():
            lone[j] = rbuf[LX + j]
            sbuf[j] = lown[j] + mine[:1] * rbuf[LX + j]
            done_dec[j] = theirs

        @pl.when(core == 1)
        def _():
            lone[j] = lown[j]
            sbuf[j] = rbuf[LX + j] + theirs[:1] * lown[j]
            done_dec[j] = mine

    for load in loads[2:]:
        load.wait()

    tiles = rows_n // TILE

    def block(h, r):
        hs = cols(h)
        at = slice(r * TILE, (r + 1) * TILE)
        extent = (r + 1) * TILE
        qt, gt = q[at, hs], g[at, hs]
        ks, vs = k[:extent, hs], v[:extent, hs]
        bt = bcol[h, at, :]
        weights = []
        for n in range(extent // 128):
            gap = bt - brow[h, :1, pl.ds(n * 128, 128)]
            weight = jnp.exp(jnp.minimum(gap, 0.0))
            if (n + 1) * 128 > r * TILE:
                ti = lax.broadcasted_iota(jnp.int32, gap.shape, 0) + r * TILE
                si = lax.broadcasted_iota(jnp.int32, gap.shape, 1) + n * 128
                weight = jnp.where(ti >= si, weight, 0.0)
            weights.append(weight)
        weight = jnp.concatenate(weights, axis=1)
        probs = (dot(qt, ks, NT) * scale * weight).astype(BF16)
        gscores = (dot(gt, vs, NT) * scale * weight).astype(BF16)
        start = wide(scale * jnp.exp(bt))
        dqt = dot(gscores, ks, NN) + dot(gt, st[h], NT) * start
        dq[at, hs] = dqt.astype(BF16)
        dkp = dot(gscores, qt, TN)
        dvp = dot(probs, gt, TN)
        if r:
            dkacc[: r * TILE, hs] += dkp[: r * TILE]
            dvacc[: r * TILE, hs] += dvp[: r * TILE]
        dkacc[at, hs] = dkp[r * TILE :]
        dvacc[at, hs] = dvp[r * TILE :]

    def finish(j, c, grad):
        at = rows(c)
        alt = lone[j, at] + done_dec[j, :1] * grad
        first = core == 0
        gin[2 * core + j, at] = jnp.where(first, alt, grad).astype(BF16)
        fs[j, at] = jnp.where(first, grad, alt)
        send(fs.at[j], FF + j, c, partner)

    owners = [n * line // PIECES for n in range(PIECES)]
    from_high = [PER_PIECE * n for n in range(PIECES)]
    from_low = [PER_PIECE * (PIECES - 1 - n) for n in range(PIECES)]
    own_at = []
    for n, own in enumerate(owners):
        reach = []
        if own < line - 1:
            reach.append(from_high[n] + DELAY * (line - 1 - own))
        if own > 0:
            reach.append(from_low[n] + DELAY * own)
        own_at.append(max(reach))

    def piece(n, t):
        j, own = n // 2, owners[n]
        base = (n % 2) * PER_PIECE

        def when(start):
            c = t - start
            return c, (c >= 0) & (c < PER_PIECE)

        c, ok = when(own_at[n] + DELAY * (steps + jnp.abs(p - own)))
        cg = base + c
        at = rows(cg)

        if own < line - 1:

            @pl.when(ok & (p > own))
            def _():
                recv(RU + j, cg)

                @pl.when(p < line - 1)
                def _():
                    send(rbuf.at[RU + j], RU + j, cg, up)
                    finish(j, cg, rbuf[FA + j, at] + rdec[DA + n, :1] * rbuf[RU + j, at])

                @pl.when(p == line - 1)
                def _():
                    finish(j, cg, rbuf[RU + j, at])

        if own > 0:

            @pl.when(ok & (p < own))
            def _():
                recv(RD + j, cg)

                @pl.when(p > 0)
                def _():
                    gsend[j, at] = sbuf[j, at] + dchip[j, :1] * rbuf[RD + j, at]
                    send(gsend.at[j], RD + j, cg, down)

                finish(j, cg, rbuf[RD + j, at])

        for s in reversed(range(steps)):
            c, ok = when(own_at[n] + DELAY * (1 + s))

            @pl.when(ok & (p == own))
            def _():
                cg = base + c
                at = rows(cg)
                later = (col // (2**s)) % 2 == 0

                @pl.when(c == 0)
                def _():
                    recv_decay(DX + s)
                    oafter[s + 1] = jnp.where(later, oafter[s] * rdec[DX + s], oafter[s])
                    if s < steps - 1:
                        xdec[s + 1] = xdec[s] * rdec[DX + s]
                        decay_copy(xdec.at[s + 1], DX + s + 1, across[s + 1]).start()

                recv(FX + s, cg)
                theirs, mine = rbuf[FX + s, at], xs[s, at]
                total = obuf[at] + jnp.where(later, oafter[s, :1] * theirs, 0.0)
                obuf[at] = total
                if s < steps - 1:
                    xs[s + 1, at] = jnp.where(
                        later, mine + xdec[s, :1] * theirs, theirs + rdec[DX + s, :1] * mine
                    )
                    send(xs.at[s + 1], FX + s + 1, cg, across[s + 1])
                else:
                    if own < line - 1:
                        send(obuf, RU + j, cg, up)
                        grad = rbuf[FA + j, at] + rdec[DA + n, :1] * total
                    else:
                        grad = total
                    if own > 0:
                        gsend[j, at] = sbuf[j, at] + dchip[j, :1] * grad
                        send(gsend.at[j], RD + j, cg, down)
                    finish(j, cg, grad)

        if own < line - 1:
            c, ok = when(from_high[n] + DELAY * (line - 1 - p))

            @pl.when(ok & (p > own))
            def _():
                cg = base + c
                at = rows(cg)

                @pl.when(p < line - 1)
                def _():
                    @pl.when(c == 0)
                    def _():
                        recv_decay(DA + n)
                        tdec[n] = dchip[j] * rdec[DA + n]

                    recv(FA + j, cg)
                    tbuf[j, at] = sbuf[j, at] + dchip[j, :1] * rbuf[FA + j, at]

                @pl.when(p == line - 1)
                def _():
                    @pl.when(c == 0)
                    def _():
                        tdec[n] = dchip[j]

                    tbuf[j, at] = sbuf[j, at]

                @pl.when(c == 0)
                def _():
                    decay_copy(tdec.at[n], DA + n, down).start()

                send(tbuf.at[j], FA + j, cg, down)

        if own > 0:
            c, ok = when(from_low[n] + DELAY * p)

            @pl.when(ok & (p < own))
            def _():
                cg = base + c
                at = rows(cg)

                @pl.when(p > 0)
                def _():
                    @pl.when(c == 0)
                    def _():
                        recv_decay(DB + n)
                        tdec[n] = dchip[j] * rdec[DB + n]

                    recv(FB + j, cg)
                    tbuf[j, at] = rbuf[FB + j, at] + rdec[DB + n, :1] * sbuf[j, at]

                @pl.when(p == 0)
                def _():
                    @pl.when(c == 0)
                    def _():
                        tdec[n] = dchip[j]

                    tbuf[j, at] = sbuf[j, at]

                @pl.when(c == 0)
                def _():
                    decay_copy(tdec.at[n], DB + n, up).start()

                send(tbuf.at[j], FB + j, cg, up)

        c, ok = when(own_at[n])

        @pl.when(ok & (p == own))
        def _():
            cg = base + c
            at = rows(cg)

            @pl.when(c == 0)
            def _():
                decay = dchip[j]
                if own < line - 1:
                    recv_decay(DA + n)
                    decay = decay * rdec[DA + n]
                if own > 0:
                    recv_decay(DB + n)
                    decay = decay * rdec[DB + n]
                xdec[0] = decay
                oafter[0] = jnp.ones_like(oafter[0])
                decay_copy(xdec.at[0], DX, across[0]).start()

            whole = sbuf[j, at]
            if own < line - 1:
                recv(FA + j, cg)
                whole = whole + dchip[j, :1] * rbuf[FA + j, at]
            if own > 0:
                recv(FB + j, cg)
                whole = rbuf[FB + j, at] + rdec[DB + n, :1] * whole
            xs[0, at] = whole
            obuf[at] = jnp.zeros((rc, hd), F32)
            send(xs.at[0], FX, cg, across[0])

    def step(t, carry):
        for n in range(PIECES):
            piece(n, t)

        for r in range(tiles):

            @pl.when((t < heads * tiles) & (t % tiles == r))
            def _():
                block(t // tiles, r)

        return carry

    last = max(
        own_at[n] + DELAY * (steps + max(own, line - 1 - own)) for n, own in enumerate(owners)
    )
    lax.fori_loop(0, max(last + PER_PIECE, heads * tiles), step, 0)

    def final(h):
        hs = cols(h)
        to_end = wide(jnp.exp(bend[h, :1] - bcol[h]))
        dk[:, hs] = (dkacc[:, hs] + dot(v[:, hs], gin[h], NT) * to_end).astype(BF16)
        dv[:, hs] = (dvacc[:, hs] + dot(k[:, hs], gin[h], NN) * to_end).astype(BF16)

    for j in range(2):
        final(2 * core + j)
    for j in range(2):
        for c in range(CHUNKS):
            recv(FF + j, c)
        gin[2 * (1 - core) + j] = rbuf[FF + j].astype(BF16)
        final(2 * (1 - core) + j)

    def sent(flow, src, base, count):
        for c in range(base, base + count):
            chunk_copy(src, flow, c, partner).wait_send()

    for j in range(2):
        decay_copy(ldec.at[j], DL + j, partner).wait_send()
        head_copy(lsend.at[j], LX + j, partner).wait_send()
        sent(FF + j, fs.at[j], 0, CHUNKS)

    for n, own in enumerate(owners):
        j, base = n // 2, (n % 2) * PER_PIECE

        @pl.when(p > own)
        def _():
            decay_copy(tdec.at[n], DA + n, partner).wait_send()
            sent(FA + j, tbuf.at[j], base, PER_PIECE)

        @pl.when(p < own)
        def _():
            decay_copy(tdec.at[n], DB + n, partner).wait_send()
            sent(FB + j, tbuf.at[j], base, PER_PIECE)

        @pl.when((p >= own) & (p < line - 1))
        def _():
            sent(RU + j, obuf, base, PER_PIECE)

        @pl.when((p <= own) & (p > 0))
        def _():
            sent(RD + j, gsend.at[j], base, PER_PIECE)

        @pl.when(p == own)
        def _():
            for s in range(steps):
                decay_copy(xdec.at[s], DX + s, partner).wait_send()
                sent(FX + s, xs.at[s], base, PER_PIECE)


def solution(mesh):
    sizes = tuple(mesh.shape[a] for a in ("gx", "gy", "gz"))
    gx, gy, gz = sizes
    line = gz // 2 if gz > 2 else gy
    columns = gx * gy * gz // (2 * line)
    steps = columns.bit_length() - 1
    assert line % PIECES == 0 and columns == 2**steps and steps >= 1

    def body(queries, keys, values, out_grad, log_decay, saved_states):
        n, width = queries.shape
        heads = log_decay.shape[0]
        hd = width // heads
        assert heads == 4
        flows = FX + steps
        hbm = pl.BlockSpec(memory_space=pltpu.HBM)
        state = (hd, hd)
        tile = (8, hd)
        out = jax.ShapeDtypeStruct((n, width), BF16)
        vm = pltpu.VMEM
        return pl.pallas_call(
            functools.partial(kernel, sizes, line, steps),
            out_shape=(out, out, out),
            in_specs=[hbm] * 4 + [pl.BlockSpec(memory_space=pltpu.VMEM), hbm],
            out_specs=(pl.BlockSpec(memory_space=pltpu.VMEM),) * 3,
            scratch_shapes=[
                vm((n, width), BF16), vm((n, width), BF16), vm((n, width), BF16), vm((n, width), BF16),
                vm((heads,) + state, BF16),
                vm((n, width), F32), vm((n, width), F32),
                vm((heads, 8, n), F32), vm((heads, n, 128), F32), vm((heads, 8, 128), F32), vm((heads,) + tile, F32),
                vm((heads,) + state, BF16),
                vm((flows,) + state, F32), vm((DX + steps,) + tile, F32),
                vm((2,) + state, F32), vm((2,) + tile, F32),
                vm((2,) + state, F32), vm((2,) + state, F32), vm((2,) + state, F32),
                vm((2,) + tile, F32), vm((2,) + tile, F32),
                vm((2,) + state, F32), vm((PIECES,) + tile, F32),
                vm((steps,) + state, F32), vm((steps,) + tile, F32), vm((steps + 1,) + tile, F32),
                vm(state, F32), vm((2,) + state, F32), vm((2,) + state, F32),
                pltpu.SemaphoreType.DMA((5,)),
                pltpu.SemaphoreType.DMA((flows, CHUNKS)), pltpu.SemaphoreType.DMA((flows, CHUNKS)),
                pltpu.SemaphoreType.DMA((DX + steps,)), pltpu.SemaphoreType.DMA((DX + steps,)),
            ],
            compiler_params=pltpu.CompilerParams(
                collective_id=0, has_side_effects=True, vmem_limit_bytes=50 * 1024 * 1024
            ),
        )(queries, keys, values, out_grad, log_decay, saved_states)

    seq = ("gx", "gy", "gz")
    return jax.shard_map(
        body,
        mesh=mesh,
        in_specs=(P(seq, None),) * 4 + (P(None, seq), P(seq, None, None, None)),
        out_specs=(P(seq, None),) * 3,
        check_vma=False,
    )
```

```python
import functools

import jax
import jax.numpy as jnp
from jax import lax
from jax.experimental import pallas as pl
from jax.experimental.pallas import tpu as pltpu
from jax.sharding import PartitionSpec as P

MESH = pl.DeviceIdType.MESH
F32 = jnp.float32
BF16 = jnp.bfloat16
PIECES = 4
PER_PIECE = 4
DELAY = 4
TILE = 256
NT = (((1,), (1,)), ((), ()))
TN = (((0,), (0,)), ((), ()))
NN = (((1,), (0,)), ((), ()))
LX, FA, FB, RU, RD, FF, FX = 0, 2, 4, 6, 8, 10, 12
DL, DA, DB, DX = 0, 2, 2 + PIECES, 2 + 2 * PIECES
CHUNKS = PIECES * PER_PIECE // 2


def dot(a, b, dims):
    return lax.dot_general(a, b, dims, preferred_element_type=F32)


def kernel(
    sizes, line, steps,
    q_hbm, k_hbm, v_hbm, g_hbm, ld_ref, st_hbm,
    dq, dk, dv,
    q, k, v, g, st, dkacc, dvacc,
    brow, bcol, bend, dvm, gin,
    rbuf, rdec, lsend, ldec, lone, lown, sbuf, done_dec, dchip, tbuf, tdec, xs, xdec, oafter, obuf, gsend, fs,
    in_sem, send_sem, recv_sem, dsend_sem, drecv_sem,
):
    gx, gy, gz = sizes
    rows_n, width = q.shape
    heads = ld_ref.shape[0]
    hd = width // heads
    scale = hd ** (-0.5)
    rc = hd // CHUNKS

    lin = (lax.axis_index("gx") * gy + lax.axis_index("gy")) * gz + lax.axis_index("gz")
    core = lin % 2
    chip = lin // 2
    p = chip % line
    col = chip // line

    def dev(core_, p_, col_):
        at = (col_ * line + p_) * 2 + core_
        return (at // (gy * gz), (at // gz) % gy, at % gz)

    def column_partner(s):
        bit = (col // (2**s)) % 2
        return col + (1 - 2 * bit) * (2**s)

    partner = dev(1 - core, p, col)
    up = dev(core, jnp.minimum(p + 1, line - 1), col)
    down = dev(core, jnp.maximum(p - 1, 0), col)
    across = [dev(core, p, column_partner(s)) for s in range(steps)]

    loads = [
        pltpu.make_async_copy(a, b, in_sem.at[n])
        for n, (a, b) in enumerate(
            [(q_hbm, q), (g_hbm, g), (k_hbm, k), (v_hbm, v), (st_hbm.at[0], st)]
        )
    ]
    for load in loads:
        load.start()

    barrier = pltpu.get_barrier_semaphore()

    def greet(to):
        pl.semaphore_signal(barrier, inc=1, device_id=to, device_id_type=MESH)

    greet(partner)
    for s in range(steps):
        greet(across[s])

    @pl.when(p > 0)
    def _():
        greet(down)

    @pl.when(p < line - 1)
    def _():
        greet(up)

    x = ld_ref[...]
    x = jnp.concatenate([x] * (8 // heads), axis=0)
    lane = lax.broadcasted_iota(jnp.int32, x.shape, 1)
    shift = 1
    while shift < rows_n:
        x = x + jnp.where(lane >= shift, pltpu.roll(x, shift, 1), 0.0)
        shift *= 2
    columns = x.T
    end = x[:, rows_n - 1 :]
    for h in range(heads):
        bcol[h] = jnp.broadcast_to(columns[:, h : h + 1], (rows_n, 128))
        bend[h] = jnp.broadcast_to(end[h : h + 1, :], (8, 128))
        brow[h] = jnp.broadcast_to(x[h : h + 1, :], (8, rows_n))
        dvm[h] = jnp.broadcast_to(jnp.exp(end[h : h + 1, :]), (8, hd))

    def wide(a):
        return jnp.concatenate([a] * (hd // 128), axis=1)

    def cols(h):
        return pl.ds(pl.multiple_of(h * hd, hd), hd)

    def local(h):
        start = wide(scale * jnp.exp(bcol[h]))
        decayed = (q[:, cols(h)].astype(F32) * start).astype(BF16)
        return dot(decayed, g[:, cols(h)], TN)

    def decay_of(h):
        return dvm[h]

    def rows(c):
        return pl.ds(pl.multiple_of(c * rc, rc), rc)

    def chunk_copy(src, flow, c, to):
        return pltpu.make_async_remote_copy(
            src_ref=src.at[rows(c)], dst_ref=rbuf.at[flow, rows(c)],
            send_sem=send_sem.at[flow, c], recv_sem=recv_sem.at[flow, c],
            device_id=to, device_id_type=MESH,
        )

    def decay_copy(src, flow, to):
        return pltpu.make_async_remote_copy(
            src_ref=src, dst_ref=rdec.at[flow],
            send_sem=dsend_sem.at[flow], recv_sem=drecv_sem.at[flow],
            device_id=to, device_id_type=MESH,
        )

    def head_copy(src, flow, to):
        return pltpu.make_async_remote_copy(
            src_ref=src, dst_ref=rbuf.at[flow],
            send_sem=send_sem.at[flow, 0], recv_sem=recv_sem.at[flow, 0],
            device_id=to, device_id_type=MESH,
        )

    def send(src, flow, c, to):
        chunk_copy(src, flow, c, to).start()

    def recv(flow, c):
        chunk_copy(rbuf.at[flow], flow, c, partner).wait_recv()

    def recv_decay(flow):
        decay_copy(rdec.at[flow], flow, partner).wait_recv()

    loads[0].wait()
    loads[1].wait()
    for j in range(2):
        other = 2 * (1 - core) + j
        lsend[j] = local(other)
        ldec[j] = decay_of(other)
        if j == 0:
            ends = (p > 0).astype(jnp.int32) + (p < line - 1).astype(jnp.int32)
            pl.semaphore_wait(barrier, 1 + steps + ends)

        decay_copy(ldec.at[j], DL + j, partner).start()
        head_copy(lsend.at[j], LX + j, partner).start()
    for j in range(2):
        lown[j] = local(2 * core + j)
    for j in range(2):
        mine = decay_of(2 * core + j)
        decay_copy(ldec.at[j], DL + j, partner).wait_recv()
        head_copy(lsend.at[j], LX + j, partner).wait_recv()
        theirs = rdec[DL + j]
        dchip[j] = mine * theirs

        @pl.when(core == 0)
        def _():
            lone[j] = rbuf[LX + j]
            sbuf[j] = lown[j] + mine[:1] * rbuf[LX + j]
            done_dec[j] = theirs

        @pl.when(core == 1)
        def _():
            lone[j] = lown[j]
            sbuf[j] = rbuf[LX + j] + theirs[:1] * lown[j]
            done_dec[j] = mine

    for load in loads[2:]:
        load.wait()

    tiles = rows_n // TILE

    def block(h, r):
        hs = cols(h)
        at = slice(r * TILE, (r + 1) * TILE)
        extent = (r + 1) * TILE
        qt, gt = q[at, hs], g[at, hs]
        ks, vs = k[:extent, hs], v[:extent, hs]
        bt = bcol[h, at, :]
        weights = []
        for n in range(extent // 128):
            gap = bt - brow[h, :1, pl.ds(n * 128, 128)]
            weight = jnp.exp(jnp.minimum(gap, 0.0))
            if (n + 1) * 128 > r * TILE:
                ti = lax.broadcasted_iota(jnp.int32, gap.shape, 0) + r * TILE
                si = lax.broadcasted_iota(jnp.int32, gap.shape, 1) + n * 128
                weight = jnp.where(ti >= si, weight, 0.0)
            weights.append(weight)
        weight = jnp.concatenate(weights, axis=1)
        probs = (dot(qt, ks, NT) * scale * weight).astype(BF16)
        gscores = (dot(gt, vs, NT) * scale * weight).astype(BF16)
        start = wide(scale * jnp.exp(bt))
        dqt = dot(gscores, ks, NN) + dot(gt, st[h], NT) * start
        dq[at, hs] = dqt.astype(BF16)
        dkp = dot(gscores, qt, TN)
        dvp = dot(probs, gt, TN)
        if r:
            dkacc[: r * TILE, hs] += dkp[: r * TILE]
            dvacc[: r * TILE, hs] += dvp[: r * TILE]
        dkacc[at, hs] = dkp[r * TILE :]
        dvacc[at, hs] = dvp[r * TILE :]

    def finish(j, c, grad):
        at = rows(c)
        alt = lone[j, at] + done_dec[j, :1] * grad
        first = core == 0
        gin[2 * core + j, at] = jnp.where(first, alt, grad).astype(BF16)
        fs[j, at] = jnp.where(first, grad, alt)
        send(fs.at[j], FF + j, c, partner)

    owners = [n * line // PIECES for n in range(PIECES)]
    from_high = [PER_PIECE * n for n in range(PIECES)]
    from_low = [PER_PIECE * (PIECES - 1 - n) for n in range(PIECES)]
    own_at = []
    for n, own in enumerate(owners):
        reach = []
        if own < line - 1:
            reach.append(from_high[n] + DELAY * (line - 1 - own))
        if own > 0:
            reach.append(from_low[n] + DELAY * own)
        own_at.append(max(reach))

    def piece(n, t):
        j, own = n // 2, owners[n]
        base = (n % 2) * PER_PIECE

        def when(start):
            c = t - start
            return c, (c >= 0) & (c < PER_PIECE)

        c, ok = when(own_at[n] + DELAY * (steps + jnp.abs(p - own)))
        cg = base + c
        at = rows(cg)

        if own < line - 1:

            @pl.when(ok & (p > own))
            def _():
                recv(RU + j, cg)

                @pl.when(p < line - 1)
                def _():
                    send(rbuf.at[RU + j], RU + j, cg, up)
                    finish(j, cg, rbuf[FA + j, at] + rdec[DA + n, :1] * rbuf[RU + j, at])

                @pl.when(p == line - 1)
                def _():
                    finish(j, cg, rbuf[RU + j, at])

        if own > 0:

            @pl.when(ok & (p < own))
            def _():
                recv(RD + j, cg)

                @pl.when(p > 0)
                def _():
                    gsend[j, at] = sbuf[j, at] + dchip[j, :1] * rbuf[RD + j, at]
                    send(gsend.at[j], RD + j, cg, down)

                finish(j, cg, rbuf[RD + j, at])

        for s in reversed(range(steps)):
            c, ok = when(own_at[n] + DELAY * (1 + s))

            @pl.when(ok & (p == own))
            def _():
                cg = base + c
                at = rows(cg)
                later = (col // (2**s)) % 2 == 0

                @pl.when(c == 0)
                def _():
                    recv_decay(DX + s)
                    oafter[s + 1] = jnp.where(later, oafter[s] * rdec[DX + s], oafter[s])
                    if s < steps - 1:
                        xdec[s + 1] = xdec[s] * rdec[DX + s]
                        decay_copy(xdec.at[s + 1], DX + s + 1, across[s + 1]).start()

                recv(FX + s, cg)
                theirs, mine = rbuf[FX + s, at], xs[s, at]
                total = obuf[at] + jnp.where(later, oafter[s, :1] * theirs, 0.0)
                obuf[at] = total
                if s < steps - 1:
                    xs[s + 1, at] = jnp.where(
                        later, mine + xdec[s, :1] * theirs, theirs + rdec[DX + s, :1] * mine
                    )
                    send(xs.at[s + 1], FX + s + 1, cg, across[s + 1])
                else:
                    if own < line - 1:
                        send(obuf, RU + j, cg, up)
                        grad = rbuf[FA + j, at] + rdec[DA + n, :1] * total
                    else:
                        grad = total
                    if own > 0:
                        gsend[j, at] = sbuf[j, at] + dchip[j, :1] * grad
                        send(gsend.at[j], RD + j, cg, down)
                    finish(j, cg, grad)

        if own < line - 1:
            c, ok = when(from_high[n] + DELAY * (line - 1 - p))

            @pl.when(ok & (p > own))
            def _():
                cg = base + c
                at = rows(cg)

                @pl.when(p < line - 1)
                def _():
                    @pl.when(c == 0)
                    def _():
                        recv_decay(DA + n)
                        tdec[n] = dchip[j] * rdec[DA + n]

                    recv(FA + j, cg)
                    tbuf[j, at] = sbuf[j, at] + dchip[j, :1] * rbuf[FA + j, at]

                @pl.when(p == line - 1)
                def _():
                    @pl.when(c == 0)
                    def _():
                        tdec[n] = dchip[j]

                    tbuf[j, at] = sbuf[j, at]

                @pl.when(c == 0)
                def _():
                    decay_copy(tdec.at[n], DA + n, down).start()

                send(tbuf.at[j], FA + j, cg, down)

        if own > 0:
            c, ok = when(from_low[n] + DELAY * p)

            @pl.when(ok & (p < own))
            def _():
                cg = base + c
                at = rows(cg)

                @pl.when(p > 0)
                def _():
                    @pl.when(c == 0)
                    def _():
                        recv_decay(DB + n)
                        tdec[n] = dchip[j] * rdec[DB + n]

                    recv(FB + j, cg)
                    tbuf[j, at] = rbuf[FB + j, at] + rdec[DB + n, :1] * sbuf[j, at]

                @pl.when(p == 0)
                def _():
                    @pl.when(c == 0)
                    def _():
                        tdec[n] = dchip[j]

                    tbuf[j, at] = sbuf[j, at]

                @pl.when(c == 0)
                def _():
                    decay_copy(tdec.at[n], DB + n, up).start()

                send(tbuf.at[j], FB + j, cg, up)

        c, ok = when(own_at[n])

        @pl.when(ok & (p == own))
        def _():
            cg = base + c
            at = rows(cg)

            @pl.when(c == 0)
            def _():
                decay = dchip[j]
                if own < line - 1:
                    recv_decay(DA + n)
                    decay = decay * rdec[DA + n]
                if own > 0:
                    recv_decay(DB + n)
                    decay = decay * rdec[DB + n]
                xdec[0] = decay
                oafter[0] = jnp.ones_like(oafter[0])
                decay_copy(xdec.at[0], DX, across[0]).start()

            whole = sbuf[j, at]
            if own < line - 1:
                recv(FA + j, cg)
                whole = whole + dchip[j, :1] * rbuf[FA + j, at]
            if own > 0:
                recv(FB + j, cg)
                whole = rbuf[FB + j, at] + rdec[DB + n, :1] * whole
            xs[0, at] = whole
            obuf[at] = jnp.zeros((rc, hd), F32)
            send(xs.at[0], FX, cg, across[0])

    def step(t, carry):
        for n in range(PIECES):
            piece(n, t)

        for r in range(tiles):

            @pl.when((t < 2 * heads * tiles) & (t % (2 * tiles) == 2 * r))
            def _():
                block(t // (2 * tiles), r)

        return carry

    last = max(
        own_at[n] + DELAY * (steps + max(own, line - 1 - own)) for n, own in enumerate(owners)
    )
    lax.fori_loop(0, max(last + PER_PIECE, heads * tiles), step, 0)

    def final(h):
        hs = cols(h)
        to_end = wide(jnp.exp(bend[h, :1] - bcol[h]))
        dk[:, hs] = (dkacc[:, hs] + dot(v[:, hs], gin[h], NT) * to_end).astype(BF16)
        dv[:, hs] = (dvacc[:, hs] + dot(k[:, hs], gin[h], NN) * to_end).astype(BF16)

    for j in range(2):
        final(2 * core + j)
    for j in range(2):
        for c in range(CHUNKS):
            recv(FF + j, c)
        gin[2 * (1 - core) + j] = rbuf[FF + j].astype(BF16)
        final(2 * (1 - core) + j)

    def sent(flow, src, base, count):
        for c in range(base, base + count):
            chunk_copy(src, flow, c, partner).wait_send()

    for j in range(2):
        decay_copy(ldec.at[j], DL + j, partner).wait_send()
        head_copy(lsend.at[j], LX + j, partner).wait_send()
        sent(FF + j, fs.at[j], 0, CHUNKS)

    for n, own in enumerate(owners):
        j, base = n // 2, (n % 2) * PER_PIECE

        @pl.when(p > own)
        def _():
            decay_copy(tdec.at[n], DA + n, partner).wait_send()
            sent(FA + j, tbuf.at[j], base, PER_PIECE)

        @pl.when(p < own)
        def _():
            decay_copy(tdec.at[n], DB + n, partner).wait_send()
            sent(FB + j, tbuf.at[j], base, PER_PIECE)

        @pl.when((p >= own) & (p < line - 1))
        def _():
            sent(RU + j, obuf, base, PER_PIECE)

        @pl.when((p <= own) & (p > 0))
        def _():
            sent(RD + j, gsend.at[j], base, PER_PIECE)

        @pl.when(p == own)
        def _():
            for s in range(steps):
                decay_copy(xdec.at[s], DX + s, partner).wait_send()
                sent(FX + s, xs.at[s], base, PER_PIECE)


def solution(mesh):
    sizes = tuple(mesh.shape[a] for a in ("gx", "gy", "gz"))
    gx, gy, gz = sizes
    line = gz // 2 if gz > 2 else gy
    columns = gx * gy * gz // (2 * line)
    steps = columns.bit_length() - 1
    assert line % PIECES == 0 and columns == 2**steps and steps >= 1

    def body(queries, keys, values, out_grad, log_decay, saved_states):
        n, width = queries.shape
        heads = log_decay.shape[0]
        hd = width // heads
        assert heads == 4
        flows = FX + steps
        hbm = pl.BlockSpec(memory_space=pltpu.HBM)
        state = (hd, hd)
        tile = (8, hd)
        out = jax.ShapeDtypeStruct((n, width), BF16)
        vm = pltpu.VMEM
        return pl.pallas_call(
            functools.partial(kernel, sizes, line, steps),
            out_shape=(out, out, out),
            in_specs=[hbm] * 4 + [pl.BlockSpec(memory_space=pltpu.VMEM), hbm],
            out_specs=(pl.BlockSpec(memory_space=pltpu.VMEM),) * 3,
            scratch_shapes=[
                vm((n, width), BF16), vm((n, width), BF16), vm((n, width), BF16), vm((n, width), BF16),
                vm((heads,) + state, BF16),
                vm((n, width), F32), vm((n, width), F32),
                vm((heads, 8, n), F32), vm((heads, n, 128), F32), vm((heads, 8, 128), F32), vm((heads,) + tile, F32),
                vm((heads,) + state, BF16),
                vm((flows,) + state, F32), vm((DX + steps,) + tile, F32),
                vm((2,) + state, F32), vm((2,) + tile, F32),
                vm((2,) + state, F32), vm((2,) + state, F32), vm((2,) + state, F32),
                vm((2,) + tile, F32), vm((2,) + tile, F32),
                vm((2,) + state, F32), vm((PIECES,) + tile, F32),
                vm((steps,) + state, F32), vm((steps,) + tile, F32), vm((steps + 1,) + tile, F32),
                vm(state, F32), vm((2,) + state, F32), vm((2,) + state, F32),
                pltpu.SemaphoreType.DMA((5,)),
                pltpu.SemaphoreType.DMA((flows, CHUNKS)), pltpu.SemaphoreType.DMA((flows, CHUNKS)),
                pltpu.SemaphoreType.DMA((DX + steps,)), pltpu.SemaphoreType.DMA((DX + steps,)),
            ],
            compiler_params=pltpu.CompilerParams(
                collective_id=0, has_side_effects=True, vmem_limit_bytes=50 * 1024 * 1024
            ),
        )(queries, keys, values, out_grad, log_decay, saved_states)

    seq = ("gx", "gy", "gz")
    return jax.shard_map(
        body,
        mesh=mesh,
        in_specs=(P(seq, None),) * 4 + (P(None, seq), P(seq, None, None, None)),
        out_specs=(P(seq, None),) * 3,
        check_vma=False,
    )
```
